32 devices in a mesh: seq: 8 (over y, x, core), tensor: 4 (over z).
Axes of the slice: x: 2, y: 2, z: 4, core: 2. Of those that a mesh axis runs over, the one named last changes fastest.
Arguments:
- tokens: bfloat16 [4096, 8192], P('seq', 'tensor'), may hold values from -6 to 6
- positions: int32 [4096], P('seq'), may hold values from 0 to 4095, each once
- norm_gain: float32 [8192], replicated, may hold values from 0.1 to 1.9
- w_query: bfloat16 [8192, 4096], P('seq', 'tensor'), may hold values from -0.0625 to 0.0625
- w_key: bfloat16 [8192, 1024], P('seq', 'tensor'), may hold values from -0.0625 to 0.0625
- w_value: bfloat16 [8192, 1024], P('seq', 'tensor'), may hold values from -0.0625 to 0.0625
- b_query: float32 [4096], P('tensor'), may hold values from -40 to 40
- b_key: float32 [1024], P('tensor'), may hold values from -40 to 40
- b_value: float32 [1024], P('tensor'), may hold values from -6 to 6
- w_out: bfloat16 [4096, 8192], P('tensor', 'seq'), may hold values from -0.09375 to 0.09375
Outputs:
- mixed: bfloat16 [4096, 8192], P('seq', 'tensor')
- context: bfloat16 [4096, 4096], P('seq', 'tensor')
The draws below stay inside these ranges and needn't reach their ends.
Inputs may be any that keep to these rules, and one draw needn't show every extreme that they name: positions holds every position 0 to 4095 once.
All inputs are finite; a program needn't handle non-finite values.
Results may differ from the reference program's by a relative error of at most 0.025.
Values may be sent and summed in bfloat16 or wider, within the bound.
A program may use at most 128 MiB of HBM per device.

```python
import jax
import jax.numpy as jnp
from jax import lax

D = 8192
HEADS = 32
KV_HEADS = 8
HD = 128
TOKENS = 4096


def draw_b_query(key, part):
    return jax.random.normal(jax.random.fold_in(key, 14), (HEADS * HD,), jnp.float32)


def draw_b_key(key, part):
    return jax.random.normal(jax.random.fold_in(key, 15), (KV_HEADS * HD,), jnp.float32)


def steps_of(rng, dims, cuts, low, high):
    factor_of, own = 1.0, jax.random.fold_in(rng, 6)
    for position, parts in cuts:
        steps = jnp.exp(jax.random.uniform(jax.random.fold_in(own, position), (parts,), jnp.float32, low / len(cuts), high / len(cuts)))
        factor_of = factor_of * jnp.repeat(steps, dims[position] // parts).reshape([-1 if axis == position else 1 for axis in range(len(dims))])
    return factor_of


def centred(own_key, dims, deviation, bound, split=(), held_as=jnp.bfloat16):
    loudness = steps_of(own_key, dims, split, -0.22, 0.18) if split else 1.0
    array = jax.random.normal(own_key, dims, jnp.float32) * deviation * loudness
    return jnp.minimum(jnp.maximum(array, -bound), bound).astype(held_as)


def setup_inputs(seed: int = 0) -> dict:
    splits = jax.random.split(jax.random.key(seed), 11)
    tokens = centred(splits[0], (TOKENS, D), 1.0, 6.0, ((0, 8), (1, 4)))
    positions = jax.random.permutation(splits[1], TOKENS).astype(jnp.int32)
    norm_gain = jnp.clip(1.0 + 0.18 * jax.random.normal(splits[2], (D,), jnp.float32), 0.1, 1.9)
    w_query = centred(splits[3], (D, HEADS * HD), D ** -0.5, 0.0625, ((0, 8), (1, 4)))
    w_key = centred(splits[4], (D, KV_HEADS * HD), D ** -0.5, 0.0625, ((0, 8), (1, 4)))
    w_value = centred(splits[5], (D, KV_HEADS * HD), D ** -0.5, 0.0625, ((0, 8), (1, 4)))
    b_query = draw_b_query(jax.random.fold_in(splits[10], 71), 0)
    b_key = draw_b_key(jax.random.fold_in(splits[10], 71), 0)
    b_value = centred(splits[8], (KV_HEADS * HD,), 1.0, 6.0, ((0, 4),), jnp.float32)
    w_out = centred(splits[9], (HEADS * HD, D), (HEADS * HD) ** -0.5, 0.09375, ((0, 4), (1, 8)))
    return dict(tokens=tokens, positions=positions, norm_gain=norm_gain, w_query=w_query, w_key=w_key, w_value=w_value, b_query=b_query, b_key=b_key, b_value=b_value, w_out=w_out)


NORM_EPS = 1e-06
ROPE_BASE = 1000000.0
NEG_FILL = -1e+30

def rotate(values_in, positions):
    half_dim = HD // 2
    inv_freq = ROPE_BASE ** (-jnp.arange(half_dim, dtype=jnp.float32) * 2.0 / HD)
    angles = positions.astype(jnp.float32)[:, None] * inv_freq[None, :]
    cosine = jnp.cos(angles)[:, None, :]
    sines = jnp.sin(angles)[:, None, :]
    lower_half = values_in[..., :half_dim]
    upper_half = values_in[..., half_dim:]
    return jnp.concatenate([lower_half * cosine - upper_half * sines, upper_half * cosine + lower_half * sines], -1)

def reference(tokens, positions, norm_gain, w_query, w_key, w_value, b_query, b_key, b_value, w_out):
    group = HEADS // KV_HEADS
    inputs = tokens.astype(jnp.float32)
    inverse_rms = lax.rsqrt(lax.optimization_barrier(jnp.mean(inputs * inputs, -1, keepdims=True)) + NORM_EPS)
    normed = (inputs * inverse_rms * norm_gain.astype(jnp.float32)[None, :]).astype(jnp.bfloat16)
    q_proj = jnp.dot(normed, w_query, preferred_element_type=jnp.float32) + b_query.astype(jnp.float32)[None, :]
    k_proj = jnp.dot(normed, w_key, preferred_element_type=jnp.float32) + b_key.astype(jnp.float32)[None, :]
    v_proj = jnp.dot(normed, w_value, preferred_element_type=jnp.float32) + b_value.astype(jnp.float32)[None, :]
    queries = rotate(q_proj.reshape(TOKENS, HEADS, HD), positions).astype(jnp.bfloat16)
    keys_rot = rotate(k_proj.reshape(TOKENS, KV_HEADS, HD), positions).astype(jnp.bfloat16)
    values = v_proj.astype(jnp.bfloat16).reshape(TOKENS, KV_HEADS, HD)
    queries = jnp.moveaxis(queries, 1, 0)
    keys_rot = jnp.moveaxis(keys_rot, 1, 0)
    values = jnp.moveaxis(values, 1, 0)
    allowed = positions[None, :] <= positions[:, None]
    scale = HD ** (-0.5)

    def one_head(head_index):
        q_head = lax.dynamic_index_in_dim(queries, head_index, 0, keepdims=False).astype(jnp.float32)
        kv_index = head_index // group
        k_head = lax.dynamic_index_in_dim(keys_rot, kv_index, 0, keepdims=False).astype(jnp.float32)
        v_head = lax.dynamic_index_in_dim(values, kv_index, 0, keepdims=False)
        scores = jnp.dot(q_head, k_head.T) * scale
        scores = jnp.where(allowed, scores, NEG_FILL)
        row_max = lax.optimization_barrier(jnp.max(scores, -1, keepdims=True))
        weights = jnp.where(allowed, jnp.exp(scores - row_max), 0.0)
        denominator = lax.optimization_barrier(jnp.sum(weights, -1, keepdims=True))
        numerator = jnp.dot(weights.astype(jnp.bfloat16), v_head, preferred_element_type=jnp.float32)
        return (numerator / denominator).astype(jnp.bfloat16)
    per_head = lax.map(one_head, jnp.arange(HEADS, dtype=jnp.int32))
    context = jnp.moveaxis(per_head, 0, 1).reshape(TOKENS, HEADS * HD)
    mixed = (inputs + jnp.dot(context, w_out, preferred_element_type=jnp.float32)).astype(jnp.bfloat16)
    return (mixed, context)
```

```python
import functools

import jax
import jax.numpy as jnp
from jax import lax
from jax.experimental import pallas as pl
from jax.experimental.pallas import tpu as pltpu
from jax.sharding import PartitionSpec as P


HD = 128


NORM_EPS = 1e-06
ROPE_BASE = 1000000.0
NEG_FILL = -1e30
CHUNKS = 4
MESH = pl.DeviceIdType.MESH
ANY = pl.BlockSpec(memory_space=pl.ANY)


def rotate(values_in, positions):
    half_dim = HD // 2
    inv_freq = ROPE_BASE ** (-jnp.arange(half_dim, dtype=jnp.float32) * 2.0 / HD)
    angles = positions.astype(jnp.float32)[:, None] * inv_freq[None, :]
    cosine = jnp.cos(angles)[:, None, :]
    sines = jnp.sin(angles)[:, None, :]
    lower_half = values_in[..., :half_dim]
    upper_half = values_in[..., half_dim:]
    return jnp.concatenate(
        [lower_half * cosine - upper_half * sines, upper_half * cosine + lower_half * sines], -1
    )


def gather_line_kernel(n, src, out, stage, send_sem, recv_sem, local_sem):
    me = lax.axis_index("tensor")
    width = src.shape[1]

    def slot(block):
        return out.at[:, pl.ds(pl.multiple_of(block * width, 128), width)]

    barrier = pltpu.get_barrier_semaphore()
    for other in ((me + 1) % n, (me + n - 1) % n):
        pl.semaphore_signal(barrier, inc=1, device_id={"tensor": other}, device_id_type=MESH)
    pl.semaphore_wait(barrier, 2)

    def copy(way, step, block, first, target):
        return pltpu.make_async_remote_copy(
            src_ref=src if first else slot(block),
            dst_ref=slot(block),
            send_sem=send_sem.at[way, step],
            recv_sem=recv_sem.at[way, step],
            device_id={"tensor": target},
            device_id_type=MESH,
        )

    def sends(step):
        right = (me >= step) & (me < n - 1)
        left = (me + step < n) & (me > 0)
        return (right, 0, me - step, me + 1), (left, 1, me + step, me - 1)

    for step in range(n - 1):
        for cond, way, block, target in sends(step):

            @pl.when(cond)
            def _():
                copy(way, step, block, step == 0, target).start()

        if step == 0:
            load = pltpu.make_async_copy(src, stage, local_sem.at[0])
            load.start()
            load.wait()
            store = pltpu.make_async_copy(stage, slot(me), local_sem.at[1])
            store.start()
            store.wait()

        @pl.when(me - 1 - step >= 0)
        def _():
            copy(0, step, me - 1 - step, False, me - 1).wait_recv()

        @pl.when(me + 1 + step < n)
        def _():
            copy(1, step, me + 1 + step, False, me + 1).wait_recv()

    for step in range(n - 1):
        for cond, way, block, target in sends(step):

            @pl.when(cond)
            def _():
                copy(way, step, block, step == 0, target).wait_send()


def gather_line(n, block):
    rows, width = block.shape
    return pl.pallas_call(
        functools.partial(gather_line_kernel, n),
        out_shape=jax.ShapeDtypeStruct((rows, n * width), block.dtype),
        in_specs=[ANY],
        out_specs=ANY,
        scratch_shapes=[
            pltpu.VMEM((rows, width), block.dtype),
            pltpu.SemaphoreType.DMA((2, n - 1)),
            pltpu.SemaphoreType.DMA((2, n - 1)),
            pltpu.SemaphoreType.DMA((2,)),
        ],
        compiler_params=pltpu.CompilerParams(collective_id=0, has_side_effects=True),
        cost_estimate=pl.CostEstimate(flops=10**11, bytes_accessed=3 * 10**8, transcendentals=0),
    )(block)


def gather_pairs_kernel(n, kv, pos, kv_out, pos_out, kv_stage, pos_stage, send_sem, recv_sem, local_sem):
    me = lax.axis_index("seq")
    twin = me + 1 - 2 * (me % 2)
    pairs = n // 2

    barrier = pltpu.get_barrier_semaphore()
    for other in [(me + 2 * j) % n for j in range(1, pairs)] + [twin]:
        pl.semaphore_signal(barrier, inc=1, device_id={"seq": other}, device_id_type=MESH)
    pl.semaphore_wait(barrier, pairs)

    arrays = ((kv, kv_out, kv_stage), (pos, pos_out, pos_stage))

    def copy(which, hop, j, block, own, target):
        source, dest, _ = arrays[which]
        return pltpu.make_async_remote_copy(
            src_ref=source if own else dest.at[block],
            dst_ref=dest.at[block],
            send_sem=send_sem.at[which, hop, j],
            recv_sem=recv_sem.at[which, hop, j],
            device_id={"seq": target},
            device_id_type=MESH,
        )

    for which in range(2):
        for j in range(1, pairs):
            copy(which, 0, j, me, True, (me + 2 * j) % n).start()
        copy(which, 1, 0, me, True, twin).start()
    for which in range(2):
        source, dest, stage = arrays[which]
        load = pltpu.make_async_copy(source, stage, local_sem.at[which, 0])
        load.start()
        load.wait()
        store = pltpu.make_async_copy(stage, dest.at[me], local_sem.at[which, 1])
        store.start()
        store.wait()
    for j in range(1, pairs):
        origin = (me + n - 2 * j) % n
        for which in range(2):
            copy(which, 0, j, origin, False, origin).wait_recv()
            copy(which, 1, j, origin, False, twin).start()
    for j in range(pairs):
        for which in range(2):
            copy(which, 1, j, (twin + n - 2 * j) % n, False, twin).wait_recv()
    for which in range(2):
        for j in range(1, pairs):
            copy(which, 0, j, me, True, (me + 2 * j) % n).wait_send()
        copy(which, 1, 0, me, True, twin).wait_send()
        for j in range(1, pairs):
            copy(which, 1, j, (me + n - 2 * j) % n, False, twin).wait_send()


def gather_pairs(n, kv, pos):
    sems = pltpu.SemaphoreType.DMA((2, 2, n // 2))
    return pl.pallas_call(
        functools.partial(gather_pairs_kernel, n),
        out_shape=(
            jax.ShapeDtypeStruct((n, *kv.shape), kv.dtype),
            jax.ShapeDtypeStruct((n, *pos.shape), pos.dtype),
        ),
        in_specs=[ANY, ANY],
        out_specs=(ANY, ANY),
        scratch_shapes=[
            pltpu.VMEM(kv.shape, kv.dtype),
            pltpu.VMEM(pos.shape, pos.dtype),
            sems,
            sems,
            pltpu.SemaphoreType.DMA((2, 2)),
        ],
        compiler_params=pltpu.CompilerParams(collective_id=1, has_side_effects=True),
        cost_estimate=pl.CostEstimate(flops=2 * 10**10, bytes_accessed=6 * 10**7, transcendentals=0),
    )(kv, pos)


def attend(queries, all_keys, all_values, key_pos, positions):
    scores = jnp.einsum("tgcd,sgd->gcts", queries, all_keys, preferred_element_type=jnp.float32)
    scores = scores * HD ** (-0.5)
    allowed = (key_pos[None, :] <= positions[:, None])[None, None, :, :]
    scores = jnp.where(allowed, scores, NEG_FILL)
    row_max = jnp.max(scores, -1, keepdims=True)
    weights = jnp.where(allowed, jnp.exp(scores - row_max), 0.0)
    denominator = jnp.sum(weights, -1)
    numerator = jnp.einsum(
        "gcts,sgd->gctd",
        weights.astype(jnp.bfloat16),
        all_values,
        preferred_element_type=jnp.float32,
    )
    per_head = numerator / denominator[..., None]
    return (
        jnp.transpose(per_head, (2, 0, 1, 3)).reshape(queries.shape[0], -1).astype(jnp.bfloat16)
    )


def reduce_terms(terms):
    return lax.psum_scatter(terms, "tensor", scatter_dimension=1, tiled=True)


def shards(seq, tensor, tokens, positions, norm_gain, w_query, w_key, w_value, b_query, b_key, b_value, w_out):
    tok_rows = tokens.shape[0]
    w_cat = jnp.concatenate((w_query, w_key, w_value), 1)
    b_cat = jnp.concatenate((b_query, b_key, b_value))
    w_all = lax.all_gather(w_cat, "seq", axis=0, tiled=True)
    features = gather_line(tensor, tokens)
    w_all, features, w_out = lax.optimization_barrier((w_all, features, w_out))
    inputs = features.astype(jnp.float32)
    inverse_rms = lax.rsqrt(jnp.mean(inputs * inputs, -1, keepdims=True) + NORM_EPS)
    normed = (inputs * inverse_rms * norm_gain[None, :]).astype(jnp.bfloat16)
    w_out_all = lax.all_gather(w_out, "seq", axis=1, tiled=True)
    projected = jnp.dot(normed, w_all, preferred_element_type=jnp.float32) + b_cat[None, :]
    query_cols = w_query.shape[1]
    key_cols = w_key.shape[1]
    heads_here = query_cols // HD
    kv_here = key_cols // HD
    group = heads_here // kv_here
    queries = rotate(projected[:, :query_cols].reshape(tok_rows, heads_here, HD), positions).astype(
        jnp.bfloat16
    )
    queries = queries.reshape(tok_rows, kv_here, group, HD)
    keys_rot = rotate(
        projected[:, query_cols : query_cols + key_cols].reshape(tok_rows, kv_here, HD), positions
    ).astype(jnp.bfloat16)
    values = projected[:, query_cols + key_cols :].astype(jnp.bfloat16)
    kv = jnp.concatenate((keys_rot.reshape(tok_rows, key_cols), values), 1)
    kv_all, pos_all = gather_pairs(seq, kv, jnp.broadcast_to(positions[None, :], (8, tok_rows)))
    all_keys = kv_all[:, :, :key_cols].reshape(seq * tok_rows, kv_here, HD)
    all_values = kv_all[:, :, key_cols:].reshape(seq * tok_rows, kv_here, HD)
    key_pos = pos_all[:, 0, :].reshape(seq * tok_rows)

    size = tok_rows // CHUNKS
    contexts, sums = [], []
    terms = None
    for chunk in range(CHUNKS):
        rows = slice(chunk * size, (chunk + 1) * size)
        part = queries[rows]
        if terms is not None:
            part, terms = lax.optimization_barrier((part, terms))
            sums.append(reduce_terms(terms))
        context = attend(part, all_keys, all_values, key_pos, positions[rows])
        contexts.append(context)
        terms = jnp.dot(context, w_out_all, preferred_element_type=jnp.float32).astype(jnp.bfloat16)
    sums.append(reduce_terms(terms))
    summed = jnp.concatenate(sums, 0).astype(jnp.float32)
    mixed = (tokens.astype(jnp.float32) + summed).astype(jnp.bfloat16)
    return (mixed, jnp.concatenate(contexts, 0))


def solution(mesh):
    in_specs = (
        P("seq", "tensor"),
        P("seq"),
        P(),
        P("seq", "tensor"),
        P("seq", "tensor"),
        P("seq", "tensor"),
        P("tensor"),
        P("tensor"),
        P("tensor"),
        P("tensor", "seq"),
    )
    out_specs = (P("seq", "tensor"), P("seq", "tensor"))

    def body(*args):
        return shards(mesh.shape["seq"], mesh.shape["tensor"], *args)

    return jax.shard_map(body, mesh=mesh, in_specs=in_specs, out_specs=out_specs, check_vma=False)
```
